32 devices in a mesh: batch: 8 (over y, x, core), head: 4 (over z).
Axes of the slice: x: 2, y: 2, z: 4, core: 2. Of those that a mesh axis runs over, the one named last changes fastest.
Arguments:
- inputs: bfloat16 [8, 128, 2048], P(None, 'batch', 'head'), parts along dimension 1, may hold values from -6 to 6
- in_weight: bfloat16 [2048, 4, 384], P(None, 'head'), may hold values from -0.125 to 0.125
- gate_weight: bfloat16 [2048, 4], P(None, 'head'), may hold values from -0.125 to 0.125
- gate_bias: float32 [4], P('head'), may hold values from -2 to 3
- norm_gain: float32 [512], P('head'), may hold values from 0.1 to 1.9
- out_weight: bfloat16 [512, 2048], P('head'), may hold values from -0.375 to 0.375
- inv_gram: float32 [128, 4, 128, 128], P('batch', 'head'), parts along dimension 0, may hold values from -17 to 17, as said below
- value_key: float32 [128, 4, 128, 128], P('batch', 'head'), parts along dimension 0, may hold values from -6 to 6
Outputs:
- layer_out: float32 [8, 128, 2048], P(None, 'batch', 'head'), parts along dimension 1
The draws below stay inside these ranges and needn't reach their ends.
There are 8 independent parts, one for each index of `batch`. The reference program is written for one: setup_inputs(seed, part) draws one part's arguments, and reference() takes and returns one part's arrays. A program takes and returns all parts, laid end to end along the dimension named above; an argument that names none is the same for every part. Nothing has to cross between parts.
Inputs may be any that keep to these rules, and one draw needn't show every extreme that they name: `inv_gram`: each [128, 128] matrix is symmetric positive definite.
All inputs are finite; a program needn't handle non-finite values.
Results may differ from the reference program's by a relative error of at most 0.0029.
Values may be sent and summed in bfloat16 or wider, within the bound.
A program may use at most 64 MiB of HBM per device.

```python
import jax
import jax.numpy as jnp
from jax import lax

D = 2048
DH = 128
SEQS = 16
STEPS = 8
HEADS = 4


def draw_inv_gram(key, part):
    shape = (SEQS, HEADS, DH, DH)
    entries = jnp.clip(jax.random.normal(key, shape, jnp.float32), -4.0, 4.0)
    gram_part = jnp.einsum('shij,shkj->shik', entries, entries, precision=lax.Precision.HIGHEST) / DH
    return 0.5 * jnp.eye(DH, dtype=jnp.float32) + gram_part


def draw_value_key(key, part):
    shape = (SEQS, HEADS, DH, DH)
    rising = 3.0 ** (jnp.arange(HEADS, dtype=jnp.float32) / max(HEADS - 1, 1))
    entries = jnp.clip(jax.random.normal(key, shape, jnp.float32), -4.0, 4.0)
    scales = 0.12 * jnp.broadcast_to(rising[None, :], (SEQS, HEADS))
    return entries * scales[:, :, None, None]


def raised(values, key, source, target, blocks, factor):
    owner, partner = [(jnp.arange(values.shape[dim]) // (values.shape[dim] // blocks)).reshape([-1 if axis == dim else 1 for axis in range(values.ndim)]) for dim in (source, target)]
    chosen = jax.random.permutation(key, blocks)[partner]
    strong = (owner == chosen) | (owner == (partner + blocks // 2) % blocks)
    return jnp.where(strong, factor * values, values)


def steps_of(rng, shape, split, low, high):
    loudness = 1.0
    for dim, shards_of in split:
        draws = jax.random.uniform(jax.random.fold_in(jax.random.fold_in(rng, 6), dim), (shards_of,), jnp.float32, low / len(split), high / len(split))
        loudness = loudness * jnp.repeat(jnp.exp(draws), shape[dim] // shards_of).reshape((-1,) + (1,) * (len(shape) - 1 - dim))
    return loudness


def normal_values(own_key, extent, spread, reach, cuts=(), kind=jnp.bfloat16):
    loudness = steps_of(own_key, extent, cuts, -0.22, 0.18) if cuts else 1.0
    array = jax.random.normal(own_key, extent, jnp.float32) * spread * loudness
    return jnp.minimum(jnp.maximum(array, -reach), reach).astype(kind)


def heavy_noise(rng, dims, width, reach, shards, heavy, kind=jnp.bfloat16):
    values = width * jax.random.normal(rng, dims, jnp.float32)
    if shards:
        values = values * steps_of(rng, dims, shards, -0.22, 0.18)
    return jnp.clip(raised(values, jax.random.fold_in(rng, 3), *heavy), -reach, reach).astype(kind)


def setup_inputs(seed: int = 0, part: int = 0) -> dict:
    splits = jax.random.split(jax.random.key(seed), 9)
    part_splits = jax.random.split(jax.random.fold_in(splits[8], part), 9)
    inputs = normal_values(part_splits[0], (STEPS, SEQS, D), 1.0, 6.0, ((2, 4),))
    in_weight = normal_values(splits[1], (D, HEADS, 3 * DH), D ** -0.5, 0.125, ((1, 4),))
    gate_weight = normal_values(splits[2], (D, HEADS), D ** -0.5, 0.125, ((1, 4),))
    gate_bias = jnp.clip(-2.0 + 5.0 * jax.random.uniform(splits[3], (HEADS,), jnp.float32) ** steps_of(splits[3], (HEADS,), ((0, 4),), -0.2, 0.2), -2.0, 3.0)
    norm_gain = jnp.clip(1.0 + 0.18 * jax.random.normal(splits[4], (HEADS * DH,), jnp.float32), 0.1, 1.9)
    out_weight = heavy_noise(splits[5], (HEADS * DH, D), (HEADS * DH) ** -0.5, 0.375, ((0, 4),), (0, 1, 4, 2.0))
    inv_gram = draw_inv_gram(jax.random.fold_in(jax.random.fold_in(splits[8], part), 71), part)
    value_key = draw_value_key(jax.random.fold_in(jax.random.fold_in(splits[8], part), 71), part)
    return dict(inputs=inputs, in_weight=in_weight, gate_weight=gate_weight, gate_bias=gate_bias, norm_gain=norm_gain, out_weight=out_weight, inv_gram=inv_gram, value_key=value_key)


def advance(gram_inv, memory, projected, gate, gate_bias, head_size):
    batch_rows, local_heads = gate.shape
    pieces = projected.reshape(batch_rows, local_heads, 3 * head_size)
    queries = pieces[..., :head_size]
    keys_now = pieces[..., head_size:2 * head_size]
    values_now = pieces[..., 2 * head_size:]
    forget = 0.8 + 0.2 * jax.nn.sigmoid(gate + gate_bias)
    keys_now = keys_now * lax.rsqrt(lax.optimization_barrier(jnp.sum(keys_now * keys_now, axis=-1, keepdims=True)) + 1e-06)
    queries = queries * lax.rsqrt(lax.optimization_barrier(jnp.sum(queries * queries, axis=-1, keepdims=True)) + 1e-06)
    gram_key = jnp.einsum('bhij,bhj->bhi', gram_inv, keys_now, precision=lax.Precision.HIGHEST)
    denominator = forget + lax.optimization_barrier(jnp.sum(keys_now * gram_key, axis=-1))
    gram_inv = (gram_inv - gram_key[..., :, None] * gram_key[..., None, :] / denominator[..., None, None]) / forget[..., None, None]
    memory = forget[..., None, None] * memory + values_now[..., :, None] * keys_now[..., None, :]
    gram_query = jnp.einsum('bhij,bhj->bhi', gram_inv, queries, precision=lax.Precision.HIGHEST)
    readout = jnp.einsum('bhij,bhj->bhi', memory, gram_query, precision=lax.Precision.HIGHEST)
    return (gram_inv, memory, readout.reshape(batch_rows, local_heads * head_size))

def reference(inputs, in_weight, gate_weight, gate_bias, norm_gain, out_weight, inv_gram, value_key):
    weight_flat = in_weight.reshape(D, HEADS * 3 * DH)
    gram_inv = inv_gram
    memory = value_key
    results = []
    for position in range(STEPS):
        projected = jnp.dot(inputs[position], weight_flat, preferred_element_type=jnp.float32)
        gate = jnp.dot(inputs[position], gate_weight, preferred_element_type=jnp.float32)
        gram_inv, memory, readout = advance(gram_inv, memory, projected, gate, gate_bias, DH)
        mean_square = lax.optimization_barrier(jnp.mean(readout * readout, axis=-1))
        hidden = (norm_gain * readout * lax.rsqrt(mean_square + 1e-06)[:, None]).astype(jnp.bfloat16)
        results.append(jnp.dot(hidden, out_weight, preferred_element_type=jnp.float32))
    return jnp.stack(results, axis=0)
```

```python
import functools
import math

import jax
import jax.numpy as jnp
from jax import lax
from jax.experimental import pallas as pl
from jax.experimental.pallas import tpu as pltpu
from jax.sharding import PartitionSpec as P

MESH = pl.DeviceIdType.MESH
F32 = jnp.float32
BF16 = jnp.bfloat16
CHUNKS = 4
NT = (((1,), (1,)), ((), ()))


def split(x):
    hi = x.astype(BF16)
    lo = (x - hi.astype(F32)).astype(BF16)
    return hi, lo


def rowsum(x):
    return jnp.sum(x, axis=-1, keepdims=True)


def kernel(
    n,
    group,
    x_hbm,
    w_hbm,
    gate_hbm,
    bias_ref,
    gain_ref,
    ow_hbm,
    a_hbm,
    m_hbm,
    out_ref,
    xg,
    w,
    gate,
    a32,
    m32,
    a2,
    m2,
    wout,
    pacc,
    gacc,
    kbuf,
    qbuf,
    akbuf,
    aqbuf,
    wbuf,
    robuf,
    rbuf,
    sqbuf,
    lsem,
    xs,
    xr,
    w1s,
    w1r,
    w2s,
    w2r,
    rs,
    rr,
    qs,
    qr,
):
    steps, seqs, feats = x_hbm.shape
    rows = steps * seqs
    heads_rows = ow_hbm.shape[0]
    cols = ow_hbm.shape[1] // n
    size = a_hbm.shape[1]
    me = lax.axis_index("head")
    b = lax.axis_index("batch")
    mine = lax.rem(b, group)
    base = b - mine
    slab = heads_rows // group
    span = steps // CHUNKS

    loads = [
        pltpu.make_async_copy(x_hbm, xg.at[me], lsem.at[0]),
        pltpu.make_async_copy(w_hbm, w, lsem.at[1]),
        pltpu.make_async_copy(gate_hbm, gate, lsem.at[2]),
        pltpu.make_async_copy(a_hbm, a32, lsem.at[3]),
        pltpu.make_async_copy(m_hbm, m32, lsem.at[4]),
        pltpu.make_async_copy(
            ow_hbm.at[:, pl.ds(pl.multiple_of(me * cols, cols), cols)], wout.at[me], lsem.at[5]
        ),
    ]
    for load in loads:
        load.start()

    barrier = pltpu.get_barrier_semaphore()

    @pl.when(me > 0)
    def _():
        pl.semaphore_signal(barrier, inc=1, device_id={"head": me - 1}, device_id_type=MESH)

    @pl.when(me < n - 1)
    def _():
        pl.semaphore_signal(barrier, inc=1, device_id={"head": me + 1}, device_id_type=MESH)

    for o in range(1, group):
        peer = base + lax.rem(mine + o, group)
        pl.semaphore_signal(barrier, inc=1, device_id={"batch": peer}, device_id_type=MESH)
    inner = jnp.logical_and(me > 0, me < n - 1)

    @pl.when(inner)
    def _():
        pl.semaphore_wait(barrier, group + 1)

    @pl.when(jnp.logical_not(inner))
    def _():
        pl.semaphore_wait(barrier, group)

    def xcopy(j, c, way):
        part = xg.at[j, pl.ds(c * span, span)]
        return pltpu.make_async_remote_copy(
            src_ref=part,
            dst_ref=part,
            send_sem=xs.at[way, j, c],
            recv_sem=xr.at[j, c],
            device_id={"head": me + 1 if way == 0 else me - 1},
            device_id_type=MESH,
        )

    def forward(j, c):
        @pl.when(me < n - 1)
        def _():
            xcopy(j, c, 0).start()

    def backward(j, c):
        @pl.when(me > 0)
        def _():
            xcopy(j, c, 1).start()

    loads[0].wait()
    for c in range(CHUNKS):
        forward(me, c)
        backward(me, c)

    def project(j, first):
        x = xg[j].reshape(rows, feats)
        at = pl.ds(pl.multiple_of(j * feats, feats), feats)
        part = jnp.dot(x, w[at, :], preferred_element_type=F32)
        g = jnp.broadcast_to(gate[:, at].astype(F32), (size, feats)).astype(BF16)
        gpart = lax.dot_general(x, g, NT, preferred_element_type=F32)
        if first:
            pacc[...] = part
            gacc[...] = gpart
        else:
            pacc[...] += part
            gacc[...] += gpart

    loads[1].wait()
    loads[2].wait()
    project(me, True)
    loads[3].wait()
    for s in range(seqs):
        hi, lo = split(a32[s])
        a2[s, :size, :] = hi
        a2[s, size:, :] = lo
    loads[4].wait()

    def prepare(start, stop):
        for s in range(start, stop):
            hi, lo = split(m32[s].T)
            m2[s, :size, :] = hi
            m2[s, size:, :] = lo

    per = -(-seqs // max(n - 1, 1))
    for d in range(1, n):
        for c in range(CHUNKS):

            @pl.when(me >= d)
            def _():
                xcopy(me - d, c, 0).wait_recv()
                forward(me - d, c)

            @pl.when(me + d < n)
            def _():
                xcopy(me + d, c, 0).wait_recv()
                backward(me + d, c)

        @pl.when(me >= d)
        def _():
            project(me - d, False)

        @pl.when(me + d < n)
        def _():
            project(me + d, False)

        if d < n - 1 or n == 2:
            prepare(seqs * (d - 1) // max(n - 2, 1), seqs * d // max(n - 2, 1))

    def w1copy(o):
        other = lax.rem(me + o, n)
        return pltpu.make_async_remote_copy(
            src_ref=ow_hbm.at[
                pl.ds(pl.multiple_of(mine * slab, slab), slab),
                pl.ds(pl.multiple_of(other * cols, cols), cols),
            ],
            dst_ref=wout.at[me, pl.ds(pl.multiple_of(mine * slab, slab), slab)],
            send_sem=w1s.at[o],
            recv_sem=w1r.at[o],
            device_id={"head": other},
            device_id_type=MESH,
        )

    for o in range(1, n):
        w1copy(o).start()

    p = pacc[...]
    f = 0.8 + 0.2 * jax.nn.sigmoid(gacc[...] + bias_ref[...])
    q = p[:, :size]
    k = p[:, size : 2 * size]
    v = p[:, 2 * size :]
    k = k * lax.rsqrt(rowsum(k * k) + 1e-06)
    q = q * lax.rsqrt(rowsum(q * q) + 1e-06)
    kbuf[...] = k
    qbuf[...] = q
    for s in range(seqs):
        at = pl.ds(s, steps, stride=seqs)
        hi, lo = split(jnp.concatenate([kbuf[at, :], qbuf[at, :]], axis=0))
        left = jnp.concatenate(
            [jnp.concatenate([hi, hi], axis=1), jnp.concatenate([lo, lo], axis=1)], axis=0
        )
        r = jnp.dot(left, a2[s], preferred_element_type=F32)
        r = r[: 2 * steps] + r[2 * steps :]
        akbuf[at, :] = r[:steps]
        aqbuf[at, :] = r[steps:]

    def piece(x, t):
        return x[t * seqs : (t + 1) * seqs]

    ks = [piece(k, t) for t in range(steps)]
    qs_ = [piece(q, t) for t in range(steps)]
    vs = [piece(v, t) for t in range(steps)]
    fs = [piece(f, t) for t in range(steps)]
    ak = [akbuf[t * seqs : (t + 1) * seqs, :] for t in range(steps)]
    aq = [aqbuf[t * seqs : (t + 1) * seqs, :] for t in range(steps)]
    ws = []
    for t in range(steps):
        u = ak[t]
        rd = 1.0 / (fs[t] + rowsum(ks[t] * u))
        rf = 1.0 / fs[t]
        for i in range(t + 1, steps):
            ak[i] = (ak[i] - u * (rowsum(u * ks[i]) * rd)) * rf
        for i in range(t, steps):
            aq[i] = (aq[i] - u * (rowsum(u * qs_[i]) * rd)) * rf
        ws.append(aq[t])
        wbuf[t * seqs : (t + 1) * seqs, :] = aq[t]

    for s in range(seqs):
        at = pl.ds(s, steps, stride=seqs)
        hi, lo = split(wbuf[at, :])
        hi, lo = hi.astype(F32), lo.astype(F32)
        left = jnp.concatenate(
            [jnp.concatenate([hi, hi], axis=1), jnp.concatenate([lo, lo], axis=1)], axis=0
        ).astype(BF16)
        r = jnp.dot(left, m2[s], preferred_element_type=F32)
        robuf[at, :] = r[:steps] + r[steps:]

    decay = []
    whole = None
    pieces = []
    for t in range(steps):
        decay = [x * fs[t] for x in decay] + [None]
        whole = fs[t] if whole is None else whole * fs[t]
        total = whole * robuf[t * seqs : (t + 1) * seqs, :]
        for i in range(t + 1):
            e = rowsum(ks[i] * ws[t])
            total = total + (e * vs[i] if decay[i] is None else (e * decay[i]) * vs[i])
        decay[t] = jnp.ones_like(fs[t])
        pieces.append(total)
    ro = jnp.concatenate(pieces, axis=0)
    hi, lo = split(ro * ro)
    sqbuf[me] = lax.dot_general(
        jnp.ones((8, 2 * size), BF16),
        jnp.concatenate([hi, lo], axis=1),
        NT,
        preferred_element_type=F32,
    )
    rbuf[me] = (gain_ref[...] * ro).astype(BF16)

    def share(buf, send, recv, o):
        return pltpu.make_async_remote_copy(
            src_ref=buf.at[me],
            dst_ref=buf.at[me],
            send_sem=send.at[o],
            recv_sem=recv.at[o],
            device_id={"head": lax.rem(me + o, n)},
            device_id_type=MESH,
        )

    rcopy = functools.partial(share, rbuf, rs, rr)
    qcopy = functools.partial(share, sqbuf, qs, qr)
    for o in range(1, n):
        rcopy(o).start()
        qcopy(o).start()

    def w2copy(o, i):
        source = lax.rem(me + n - o, n)
        part = wout.at[source, pl.ds(pl.multiple_of(mine * slab, slab), slab)]
        return pltpu.make_async_remote_copy(
            src_ref=part,
            dst_ref=part,
            send_sem=w2s.at[o, i],
            recv_sem=w2r.at[o, i],
            device_id={"batch": base + lax.rem(mine + i, group)},
            device_id_type=MESH,
        )

    for o in range(1, n):
        w1copy(o).wait_recv()
        for i in range(1, group):
            w2copy(o, i).start()

    loads[5].wait()
    acc = jnp.dot(rbuf[me], wout[me], preferred_element_type=F32)
    squares = sqbuf[me]
    for o in range(1, n):
        source = lax.rem(me + n - o, n)
        rcopy(o).wait_recv()
        qcopy(o).wait_recv()
        for i in range(1, group):
            w2copy(o, i).wait_recv()
        acc = acc + jnp.dot(rbuf[source], wout[source], preferred_element_type=F32)
        squares = squares + sqbuf[source]
    scale = lax.rsqrt(squares[:1] / (n * size) + 1e-06)
    scale = jnp.broadcast_to(scale, (size, rows)).T
    for at in range(0, cols, size):
        out_ref[:, at : at + size] = acc[:, at : at + size] * scale

    for d in range(n):
        for c in range(CHUNKS):

            @pl.when(jnp.logical_and(me >= d, me < n - 1))
            def _():
                xcopy(me - d, c, 0).wait_send()

            @pl.when(jnp.logical_and(me + d < n, me > 0))
            def _():
                xcopy(me + d, c, 1).wait_send()

    for o in range(1, n):
        w1copy(o).wait_send()
        rcopy(o).wait_send()
        qcopy(o).wait_send()
        for i in range(1, group):
            w2copy(o, i).wait_send()


def local(n, batch, inputs, in_weight, gate_weight, gate_bias, norm_gain, out_weight, inv_gram, value_key):
    steps, seqs, feats = inputs.shape
    d_model, heads, width = in_weight.shape
    size = width // 3
    rows = steps * seqs
    cols = out_weight.shape[1] // n
    assert heads == 1
    group = math.gcd(math.gcd(batch, 8), out_weight.shape[0] // 16)
    anywhere = pl.BlockSpec(memory_space=pl.ANY)
    vmem = pl.BlockSpec(memory_space=pltpu.VMEM)
    dma = pltpu.SemaphoreType.DMA
    out = pl.pallas_call(
        functools.partial(kernel, n, group),
        out_shape=jax.ShapeDtypeStruct((rows, cols), F32),
        in_specs=[
            anywhere,
            anywhere,
            anywhere,
            vmem,
            vmem,
            anywhere,
            anywhere,
            anywhere,
        ],
        out_specs=vmem,
        scratch_shapes=[
            pltpu.VMEM((n, steps, seqs, feats), BF16),
            pltpu.VMEM((d_model, width), BF16),
            pltpu.VMEM((1, d_model), BF16),
            pltpu.VMEM((seqs, size, size), F32),
            pltpu.VMEM((seqs, size, size), F32),
            pltpu.VMEM((seqs, 2 * size, size), BF16),
            pltpu.VMEM((seqs, 2 * size, size), BF16),
            pltpu.VMEM((n, out_weight.shape[0], cols), BF16),
            pltpu.VMEM((rows, width), F32),
            pltpu.VMEM((rows, size), F32),
            pltpu.VMEM((rows, size), F32),
            pltpu.VMEM((rows, size), F32),
            pltpu.VMEM((rows, size), F32),
            pltpu.VMEM((rows, size), F32),
            pltpu.VMEM((rows, size), F32),
            pltpu.VMEM((rows, size), F32),
            pltpu.VMEM((n, rows, size), BF16),
            pltpu.VMEM((n, 8, rows), F32),
            dma((6,)),
            dma((2, n, CHUNKS)),
            dma((n, CHUNKS)),
            dma((n,)),
            dma((n,)),
            dma((n, group)),
            dma((n, group)),
            dma((n,)),
            dma((n,)),
            dma((n,)),
            dma((n,)),
        ],
        compiler_params=pltpu.CompilerParams(collective_id=0, has_side_effects=True),
    )(
        inputs,
        in_weight.reshape(d_model, width),
        gate_weight.reshape(1, d_model),
        gate_bias.reshape(1, 1),
        norm_gain.reshape(1, size),
        out_weight,
        inv_gram.reshape(seqs, size, size),
        value_key.reshape(seqs, size, size),
    )
    return out.reshape(steps, seqs, cols)


def solution(mesh):
    in_specs = (
        P(None, "batch", "head"),
        P(None, "head", None),
        P(None, "head"),
        P("head"),
        P("head"),
        P("head", None),
        P("batch", "head", None, None),
        P("batch", "head", None, None),
    )
    out_specs = P(None, "batch", "head")
    return jax.shard_map(
        functools.partial(local, mesh.shape["head"], mesh.shape["batch"]),
        mesh=mesh,
        in_specs=in_specs,
        out_specs=out_specs,
        check_vma=False,
    )
```

```python
import functools
import math

import jax
import jax.numpy as jnp
from jax import lax
from jax.experimental import pallas as pl
from jax.experimental.pallas import tpu as pltpu
from jax.sharding import PartitionSpec as P

MESH = pl.DeviceIdType.MESH
F32 = jnp.float32
BF16 = jnp.bfloat16
NT = (((1,), (1,)), ((), ()))


def split(x):
    hi = x.astype(BF16)
    lo = (x - hi.astype(F32)).astype(BF16)
    return hi, lo


def rowsum(x):
    return jnp.sum(x, axis=-1, keepdims=True)


def kernel(
    n,
    group,
    x_hbm,
    w_hbm,
    gate_hbm,
    bias_ref,
    gain_ref,
    ow_hbm,
    a_hbm,
    m_hbm,
    out_ref,
    xg,
    w,
    gate,
    a32,
    m32,
    a2,
    m2,
    wout,
    pacc,
    gacc,
    kbuf,
    qbuf,
    akbuf,
    aqbuf,
    wbuf,
    robuf,
    rbuf,
    sqbuf,
    lsem,
    xs,
    xr,
    w1s,
    w1r,
    w2s,
    w2r,
    rs,
    rr,
    qs,
    qr,
):
    steps, seqs, feats = x_hbm.shape
    rows = steps * seqs
    heads_rows = ow_hbm.shape[0]
    cols = ow_hbm.shape[1] // n
    size = a_hbm.shape[1]
    me = lax.axis_index("head")
    b = lax.axis_index("batch")
    mine = lax.rem(b, group)
    base = b - mine
    slab = heads_rows // group

    loads = [
        pltpu.make_async_copy(x_hbm, xg.at[me], lsem.at[0]),
        pltpu.make_async_copy(w_hbm, w, lsem.at[1]),
        pltpu.make_async_copy(gate_hbm, gate, lsem.at[2]),
        pltpu.make_async_copy(a_hbm, a32, lsem.at[3]),
        pltpu.make_async_copy(m_hbm, m32, lsem.at[4]),
        pltpu.make_async_copy(
            ow_hbm.at[:, pl.ds(pl.multiple_of(me * cols, cols), cols)], wout.at[me], lsem.at[5]
        ),
    ]
    for load in loads:
        load.start()

    barrier = pltpu.get_barrier_semaphore()

    for o in range(1, n):
        pl.semaphore_signal(
            barrier, inc=1, device_id={"head": lax.rem(me + o, n)}, device_id_type=MESH
        )
    for o in range(1, group):
        peer = base + lax.rem(mine + o, group)
        pl.semaphore_signal(barrier, inc=1, device_id={"batch": peer}, device_id_type=MESH)
    pl.semaphore_wait(barrier, n + group - 2)

    order = sorted(range(1, n), key=lambda o: -min(o, n - o))

    def xcopy(o):
        return pltpu.make_async_remote_copy(
            src_ref=xg.at[me],
            dst_ref=xg.at[me],
            send_sem=xs.at[o],
            recv_sem=xr.at[o],
            device_id={"head": lax.rem(me + o, n)},
            device_id_type=MESH,
        )

    loads[0].wait()
    for o in order:
        xcopy(o).start()

    def w1copy(o):
        other = lax.rem(me + o, n)
        return pltpu.make_async_remote_copy(
            src_ref=ow_hbm.at[
                pl.ds(pl.multiple_of(mine * slab, slab), slab),
                pl.ds(pl.multiple_of(other * cols, cols), cols),
            ],
            dst_ref=wout.at[me, pl.ds(pl.multiple_of(mine * slab, slab), slab)],
            send_sem=w1s.at[o],
            recv_sem=w1r.at[o],
            device_id={"head": other},
            device_id_type=MESH,
        )

    for o in range(1, n):
        w1copy(o).start()

    def project(j, first):
        x = xg[j].reshape(rows, feats)
        at = pl.ds(pl.multiple_of(j * feats, feats), feats)
        part = jnp.dot(x, w[at, :], preferred_element_type=F32)
        g = jnp.broadcast_to(gate[:, at].astype(F32), (size, feats)).astype(BF16)
        gpart = lax.dot_general(x, g, NT, preferred_element_type=F32)
        if first:
            pacc[...] = part
            gacc[...] = gpart
        else:
            pacc[...] += part
            gacc[...] += gpart

    loads[1].wait()
    loads[2].wait()
    project(me, True)
    loads[3].wait()
    for s in range(seqs):
        hi, lo = split(a32[s])
        a2[s, :size, :] = hi
        a2[s, size:, :] = lo
    loads[4].wait()

    def prepare(start, stop):
        for s in range(start, stop):
            hi, lo = split(m32[s].T)
            m2[s, :size, :] = hi
            m2[s, size:, :] = lo

    for at, o in enumerate(order):
        xcopy(o).wait_recv()
        project(lax.rem(me + n - o, n), False)
        prepare(seqs * at // (n - 1), seqs * (at + 1) // (n - 1))

    p = pacc[...]
    f = 0.8 + 0.2 * jax.nn.sigmoid(gacc[...] + bias_ref[...])
    q = p[:, :size]
    k = p[:, size : 2 * size]
    v = p[:, 2 * size :]
    k = k * lax.rsqrt(rowsum(k * k) + 1e-06)
    q = q * lax.rsqrt(rowsum(q * q) + 1e-06)
    kbuf[...] = k
    qbuf[...] = q
    for s in range(seqs):
        at = pl.ds(s, steps, stride=seqs)
        hi, lo = split(jnp.concatenate([kbuf[at, :], qbuf[at, :]], axis=0))
        left = jnp.concatenate(
            [jnp.concatenate([hi, hi], axis=1), jnp.concatenate([lo, lo], axis=1)], axis=0
        )
        r = jnp.dot(left, a2[s], preferred_element_type=F32)
        r = r[: 2 * steps] + r[2 * steps :]
        akbuf[at, :] = r[:steps]
        aqbuf[at, :] = r[steps:]

    def piece(x, t):
        return x[t * seqs : (t + 1) * seqs]

    ks = [piece(k, t) for t in range(steps)]
    qs_ = [piece(q, t) for t in range(steps)]
    vs = [piece(v, t) for t in range(steps)]
    fs = [piece(f, t) for t in range(steps)]
    ak = [akbuf[t * seqs : (t + 1) * seqs, :] for t in range(steps)]
    aq = [aqbuf[t * seqs : (t + 1) * seqs, :] for t in range(steps)]
    ws = []
    for t in range(steps):
        u = ak[t]
        rd = 1.0 / (fs[t] + rowsum(ks[t] * u))
        rf = 1.0 / fs[t]
        for i in range(t + 1, steps):
            ak[i] = (ak[i] - u * (rowsum(u * ks[i]) * rd)) * rf
        for i in range(t, steps):
            aq[i] = (aq[i] - u * (rowsum(u * qs_[i]) * rd)) * rf
        ws.append(aq[t])
        wbuf[t * seqs : (t + 1) * seqs, :] = aq[t]

    def w2copy(o, i):
        source = lax.rem(me + n - o, n)
        part = wout.at[source, pl.ds(pl.multiple_of(mine * slab, slab), slab)]
        return pltpu.make_async_remote_copy(
            src_ref=part,
            dst_ref=part,
            send_sem=w2s.at[o, i],
            recv_sem=w2r.at[o, i],
            device_id={"batch": base + lax.rem(mine + i, group)},
            device_id_type=MESH,
        )

    for o in range(1, n):
        w1copy(o).wait_recv()
        for i in range(1, group):
            w2copy(o, i).start()

    for s in range(seqs):
        at = pl.ds(s, steps, stride=seqs)
        hi, lo = split(wbuf[at, :])
        hi, lo = hi.astype(F32), lo.astype(F32)
        left = jnp.concatenate(
            [jnp.concatenate([hi, hi], axis=1), jnp.concatenate([lo, lo], axis=1)], axis=0
        ).astype(BF16)
        r = jnp.dot(left, m2[s], preferred_element_type=F32)
        robuf[at, :] = r[:steps] + r[steps:]

    decay = []
    whole = None
    pieces = []
    for t in range(steps):
        decay = [x * fs[t] for x in decay] + [None]
        whole = fs[t] if whole is None else whole * fs[t]
        total = whole * robuf[t * seqs : (t + 1) * seqs, :]
        for i in range(t + 1):
            e = rowsum(ks[i] * ws[t])
            total = total + (e * vs[i] if decay[i] is None else (e * decay[i]) * vs[i])
        decay[t] = jnp.ones_like(fs[t])
        pieces.append(total)
    ro = jnp.concatenate(pieces, axis=0)
    hi, lo = split(ro * ro)
    sqbuf[me] = lax.dot_general(
        jnp.ones((8, 2 * size), BF16),
        jnp.concatenate([hi, lo], axis=1),
        NT,
        preferred_element_type=F32,
    )
    rbuf[me] = (gain_ref[...] * ro).astype(BF16)

    def share(buf, send, recv, o):
        return pltpu.make_async_remote_copy(
            src_ref=buf.at[me],
            dst_ref=buf.at[me],
            send_sem=send.at[o],
            recv_sem=recv.at[o],
            device_id={"head": lax.rem(me + o, n)},
            device_id_type=MESH,
        )

    rcopy = functools.partial(share, rbuf, rs, rr)
    qcopy = functools.partial(share, sqbuf, qs, qr)
    for o in range(1, n):
        rcopy(o).start()
        qcopy(o).start()

    loads[5].wait()
    acc = jnp.dot(rbuf[me], wout[me], preferred_element_type=F32)
    squares = sqbuf[me]
    for o in range(1, n):
        source = lax.rem(me + n - o, n)
        rcopy(o).wait_recv()
        qcopy(o).wait_recv()
        for i in range(1, group):
            w2copy(o, i).wait_recv()
        acc = acc + jnp.dot(rbuf[source], wout[source], preferred_element_type=F32)
        squares = squares + sqbuf[source]
    scale = lax.rsqrt(squares[:1] / (n * size) + 1e-06)
    scale = jnp.broadcast_to(scale, (size, rows)).T
    for at in range(0, cols, size):
        out_ref[:, at : at + size] = acc[:, at : at + size] * scale

    for o in range(1, n):
        xcopy(o).wait_send()
        w1copy(o).wait_send()
        rcopy(o).wait_send()
        qcopy(o).wait_send()
        for i in range(1, group):
            w2copy(o, i).wait_send()


def local(n, batch, inputs, in_weight, gate_weight, gate_bias, norm_gain, out_weight, inv_gram, value_key):
    steps, seqs, feats = inputs.shape
    d_model, heads, width = in_weight.shape
    size = width // 3
    rows = steps * seqs
    cols = out_weight.shape[1] // n
    assert heads == 1
    group = math.gcd(math.gcd(batch, 8), out_weight.shape[0] // 16)
    anywhere = pl.BlockSpec(memory_space=pl.ANY)
    vmem = pl.BlockSpec(memory_space=pltpu.VMEM)
    dma = pltpu.SemaphoreType.DMA
    out = pl.pallas_call(
        functools.partial(kernel, n, group),
        out_shape=jax.ShapeDtypeStruct((rows, cols), F32),
        in_specs=[
            anywhere,
            anywhere,
            anywhere,
            vmem,
            vmem,
            anywhere,
            anywhere,
            anywhere,
        ],
        out_specs=vmem,
        scratch_shapes=[
            pltpu.VMEM((n, steps, seqs, feats), BF16),
            pltpu.VMEM((d_model, width), BF16),
            pltpu.VMEM((1, d_model), BF16),
            pltpu.VMEM((seqs, size, size), F32),
            pltpu.VMEM((seqs, size, size), F32),
            pltpu.VMEM((seqs, 2 * size, size), BF16),
            pltpu.VMEM((seqs, 2 * size, size), BF16),
            pltpu.VMEM((n, out_weight.shape[0], cols), BF16),
            pltpu.VMEM((rows, width), F32),
            pltpu.VMEM((rows, size), F32),
            pltpu.VMEM((rows, size), F32),
            pltpu.VMEM((rows, size), F32),
            pltpu.VMEM((rows, size), F32),
            pltpu.VMEM((rows, size), F32),
            pltpu.VMEM((rows, size), F32),
            pltpu.VMEM((rows, size), F32),
            pltpu.VMEM((n, rows, size), BF16),
            pltpu.VMEM((n, 8, rows), F32),
            dma((6,)),
            dma((n,)),
            dma((n,)),
            dma((n,)),
            dma((n,)),
            dma((n, group)),
            dma((n, group)),
            dma((n,)),
            dma((n,)),
            dma((n,)),
            dma((n,)),
        ],
        compiler_params=pltpu.CompilerParams(collective_id=0, has_side_effects=True),
    )(
        inputs,
        in_weight.reshape(d_model, width),
        gate_weight.reshape(1, d_model),
        gate_bias.reshape(1, 1),
        norm_gain.reshape(1, size),
        out_weight,
        inv_gram.reshape(seqs, size, size),
        value_key.reshape(seqs, size, size),
    )
    return out.reshape(steps, seqs, cols)


def solution(mesh):
    in_specs = (
        P(None, "batch", "head"),
        P(None, "head", None),
        P(None, "head"),
        P("head"),
        P("head"),
        P("head", None),
        P("batch", "head", None, None),
        P("batch", "head", None, None),
    )
    out_specs = P(None, "batch", "head")
    return jax.shard_map(
        functools.partial(local, mesh.shape["head"], mesh.shape["batch"]),
        mesh=mesh,
        in_specs=in_specs,
        out_specs=out_specs,
        check_vma=False,
    )
```

```python
import functools
import math

import jax
import jax.numpy as jnp
from jax import lax
from jax.experimental import pallas as pl
from jax.experimental.pallas import tpu as pltpu
from jax.sharding import PartitionSpec as P

MESH = pl.DeviceIdType.MESH
F32 = jnp.float32
BF16 = jnp.bfloat16
HALVES = 2
NT = (((1,), (1,)), ((), ()))


def split(x):
    hi = x.astype(BF16)
    lo = (x - hi.astype(F32)).astype(BF16)
    return hi, lo


def rowsum(x):
    return jnp.sum(x, axis=-1, keepdims=True)


def kernel(
    n,
    group,
    x_hbm,
    w_hbm,
    gate_hbm,
    bias_ref,
    gain_ref,
    ow_hbm,
    a_hbm,
    m_hbm,
    out_ref,
    xg,
    w,
    gate,
    a32,
    m32,
    a2,
    m2,
    wout,
    pacc,
    gacc,
    kbuf,
    qbuf,
    akbuf,
    aqbuf,
    wbuf,
    robuf,
    rbuf,
    sqbuf,
    lsem,
    xs,
    xr,
    w1s,
    w1r,
    w2s,
    w2r,
    rs,
    rr,
    qs,
    qr,
):
    steps, seqs, feats = x_hbm.shape
    rows = steps * seqs
    heads_rows = ow_hbm.shape[0]
    cols = ow_hbm.shape[1] // n
    size = a_hbm.shape[1]
    me = lax.axis_index("head")
    b = lax.axis_index("batch")
    mine = lax.rem(b, group)
    base = b - mine
    slab = heads_rows // group

    loads = [
        pltpu.make_async_copy(x_hbm, xg.at[me], lsem.at[0]),
        pltpu.make_async_copy(w_hbm, w, lsem.at[1]),
        pltpu.make_async_copy(gate_hbm, gate, lsem.at[2]),
        pltpu.make_async_copy(a_hbm, a32, lsem.at[3]),
        pltpu.make_async_copy(m_hbm, m32, lsem.at[4]),
        pltpu.make_async_copy(
            ow_hbm.at[:, pl.ds(pl.multiple_of(me * cols, cols), cols)], wout.at[me], lsem.at[5]
        ),
    ]
    for load in loads:
        load.start()

    barrier = pltpu.get_barrier_semaphore()

    for o in range(1, n):
        pl.semaphore_signal(
            barrier, inc=1, device_id={"head": lax.rem(me + o, n)}, device_id_type=MESH
        )
    for o in range(1, group):
        peer = base + lax.rem(mine + o, group)
        pl.semaphore_signal(barrier, inc=1, device_id={"batch": peer}, device_id_type=MESH)
    pl.semaphore_wait(barrier, n + group - 2)

    order = sorted(range(1, n), key=lambda o: -min(o, n - o))

    part = steps // HALVES
    band = part * seqs

    def xcopy(o, h):
        block = xg.at[me, pl.ds(h * part, part)]
        return pltpu.make_async_remote_copy(
            src_ref=block,
            dst_ref=block,
            send_sem=xs.at[o, h],
            recv_sem=xr.at[o, h],
            device_id={"head": lax.rem(me + o, n)},
            device_id_type=MESH,
        )

    loads[0].wait()
    for h in range(HALVES):
        for o in order:
            xcopy(o, h).start()

    def w1copy(o):
        other = lax.rem(me + o, n)
        return pltpu.make_async_remote_copy(
            src_ref=ow_hbm.at[
                pl.ds(pl.multiple_of(mine * slab, slab), slab),
                pl.ds(pl.multiple_of(other * cols, cols), cols),
            ],
            dst_ref=wout.at[me, pl.ds(pl.multiple_of(mine * slab, slab), slab)],
            send_sem=w1s.at[o],
            recv_sem=w1r.at[o],
            device_id={"head": other},
            device_id_type=MESH,
        )

    for o in range(1, n):
        w1copy(o).start()

    def project(j, h, first):
        x = xg[j, h * part : (h + 1) * part].reshape(band, feats)
        own = slice(h * band, (h + 1) * band)
        at = pl.ds(pl.multiple_of(j * feats, feats), feats)
        partial = jnp.dot(x, w[at, :], preferred_element_type=F32)
        g = jnp.broadcast_to(gate[:, at].astype(F32), (size, feats)).astype(BF16)
        gpart = lax.dot_general(x, g, NT, preferred_element_type=F32)
        if first:
            pacc[own, :] = partial
            gacc[own, :] = gpart
        else:
            pacc[own, :] += partial
            gacc[own, :] += gpart

    loads[1].wait()
    loads[2].wait()
    for h in range(HALVES):
        project(me, h, True)
    loads[3].wait()
    for s in range(seqs):
        hi, lo = split(a32[s])
        a2[s, :size, :] = hi
        a2[s, size:, :] = lo
    loads[4].wait()

    def prepare(start, stop):
        for s in range(start, stop):
            hi, lo = split(m32[s].T)
            m2[s, :size, :] = hi
            m2[s, size:, :] = lo

    def share(buf, send, recv, o, h):
        return pltpu.make_async_remote_copy(
            src_ref=buf.at[h, me],
            dst_ref=buf.at[h, me],
            send_sem=send.at[o, h],
            recv_sem=recv.at[o, h],
            device_id={"head": lax.rem(me + o, n)},
            device_id_type=MESH,
        )

    rcopy = functools.partial(share, rbuf, rs, rr)
    qcopy = functools.partial(share, sqbuf, qs, qr)

    def w2copy(o, i):
        source = lax.rem(me + n - o, n)
        part = wout.at[source, pl.ds(pl.multiple_of(mine * slab, slab), slab)]
        return pltpu.make_async_remote_copy(
            src_ref=part,
            dst_ref=part,
            send_sem=w2s.at[o, i],
            recv_sem=w2r.at[o, i],
            device_id={"batch": base + lax.rem(mine + i, group)},
            device_id_type=MESH,
        )

    def pair(hi, lo):
        hi, lo = hi.astype(F32), lo.astype(F32)
        top = jnp.concatenate([hi, hi], axis=1)
        low = jnp.concatenate([lo, lo], axis=1)
        return jnp.concatenate([top, low], axis=0).astype(BF16)

    def piece(x, t):
        return x[t * seqs : (t + 1) * seqs]

    ks, vs, fs, us, rds, rfs = [], [], [], [], [], []
    decay = []
    whole = None
    for h in range(HALVES):
        for at, o in enumerate(order):
            xcopy(o, h).wait_recv()
            project(lax.rem(me + n - o, n), h, False)
            if h == 0:
                prepare(seqs * at // (n - 1), seqs * (at + 1) // (n - 1))

        own = slice(h * band, (h + 1) * band)
        p = pacc[own, :]
        f = 0.8 + 0.2 * jax.nn.sigmoid(gacc[own, :] + bias_ref[...])
        q = p[:, :size]
        k = p[:, size : 2 * size]
        v = p[:, 2 * size :]
        k = k * lax.rsqrt(rowsum(k * k) + 1e-06)
        q = q * lax.rsqrt(rowsum(q * q) + 1e-06)
        kbuf[own, :] = k
        qbuf[own, :] = q
        for s in range(seqs):
            at = pl.ds(h * band + s, part, stride=seqs)
            left = pair(*split(jnp.concatenate([kbuf[at, :], qbuf[at, :]], axis=0)))
            r = jnp.dot(left, a2[s], preferred_element_type=F32)
            r = r[: 2 * part] + r[2 * part :]
            akbuf[at, :] = r[:part]
            aqbuf[at, :] = r[part:]

        now = range(h * part, (h + 1) * part)
        ks += [piece(k, t) for t in range(part)]
        vs += [piece(v, t) for t in range(part)]
        fs += [piece(f, t) for t in range(part)]
        qn = {t: piece(q, t - now[0]) for t in now}
        ak = {t: akbuf[t * seqs : (t + 1) * seqs, :] for t in now}
        aq = {t: aqbuf[t * seqs : (t + 1) * seqs, :] for t in now}
        ws = {}
        for t in range(now[-1] + 1):
            if t in now:
                us.append(ak[t])
                rds.append(1.0 / (fs[t] + rowsum(ks[t] * ak[t])))
                rfs.append(1.0 / fs[t])
            u, rd, rf = us[t], rds[t], rfs[t]
            for i in now:
                if i > t:
                    ak[i] = (ak[i] - u * (rowsum(u * ks[i]) * rd)) * rf
                if i >= t:
                    aq[i] = (aq[i] - u * (rowsum(u * qn[i]) * rd)) * rf
            if t in now:
                ws[t] = aq[t]
                wbuf[t * seqs : (t + 1) * seqs, :] = aq[t]

        if h == HALVES - 1:
            for o in range(1, n):
                w1copy(o).wait_recv()
                for i in range(1, group):
                    w2copy(o, i).start()

        for s in range(seqs):
            at = pl.ds(h * band + s, part, stride=seqs)
            r = jnp.dot(pair(*split(wbuf[at, :])), m2[s], preferred_element_type=F32)
            robuf[at, :] = r[:part] + r[part:]

        pieces = []
        for t in now:
            decay = [fs[t] if x is None else x * fs[t] for x in decay] + [None]
            whole = fs[t] if whole is None else whole * fs[t]
            total = whole * robuf[t * seqs : (t + 1) * seqs, :]
            for i in range(t + 1):
                e = rowsum(ks[i] * ws[t])
                total = total + (e * vs[i] if decay[i] is None else (e * decay[i]) * vs[i])
            pieces.append(total)
        ro = jnp.concatenate(pieces, axis=0)
        hi, lo = split(ro * ro)
        squares = jnp.concatenate([hi, lo], axis=1)
        sqbuf[h, me] = lax.dot_general(
            jnp.ones((8, 2 * size), BF16),
            jnp.concatenate([squares] * HALVES, axis=0),
            NT,
            preferred_element_type=F32,
        )
        rbuf[h, me] = (gain_ref[...] * ro).astype(BF16)
        for o in range(1, n):
            rcopy(o, h).start()
            qcopy(o, h).start()

    loads[5].wait()
    for h in range(HALVES):
        acc = jnp.dot(rbuf[h, me], wout[me], preferred_element_type=F32)
        squares = sqbuf[h, me]
        for o in range(1, n):
            source = lax.rem(me + n - o, n)
            rcopy(o, h).wait_recv()
            qcopy(o, h).wait_recv()
            if h == 0:
                for i in range(1, group):
                    w2copy(o, i).wait_recv()
            acc = acc + jnp.dot(rbuf[h, source], wout[source], preferred_element_type=F32)
            squares = squares + sqbuf[h, source]
        scale = lax.rsqrt(squares[:1] / (n * size) + 1e-06)
        scale = jnp.broadcast_to(scale, (size, rows)).T[:band]
        for at in range(0, cols, size):
            out_ref[h * band : (h + 1) * band, at : at + size] = acc[:, at : at + size] * scale

    for o in range(1, n):
        w1copy(o).wait_send()
        for h in range(HALVES):
            xcopy(o, h).wait_send()
            rcopy(o, h).wait_send()
            qcopy(o, h).wait_send()
        for i in range(1, group):
            w2copy(o, i).wait_send()


def local(n, batch, inputs, in_weight, gate_weight, gate_bias, norm_gain, out_weight, inv_gram, value_key):
    steps, seqs, feats = inputs.shape
    d_model, heads, width = in_weight.shape
    size = width // 3
    rows = steps * seqs
    cols = out_weight.shape[1] // n
    assert heads == 1
    group = math.gcd(math.gcd(batch, 8), out_weight.shape[0] // 16)
    anywhere = pl.BlockSpec(memory_space=pl.ANY)
    vmem = pl.BlockSpec(memory_space=pltpu.VMEM)
    dma = pltpu.SemaphoreType.DMA
    out = pl.pallas_call(
        functools.partial(kernel, n, group),
        out_shape=jax.ShapeDtypeStruct((rows, cols), F32),
        in_specs=[
            anywhere,
            anywhere,
            anywhere,
            vmem,
            vmem,
            anywhere,
            anywhere,
            anywhere,
        ],
        out_specs=vmem,
        scratch_shapes=[
            pltpu.VMEM((n, steps, seqs, feats), BF16),
            pltpu.VMEM((d_model, width), BF16),
            pltpu.VMEM((1, d_model), BF16),
            pltpu.VMEM((seqs, size, size), F32),
            pltpu.VMEM((seqs, size, size), F32),
            pltpu.VMEM((seqs, 2 * size, size), BF16),
            pltpu.VMEM((seqs, 2 * size, size), BF16),
            pltpu.VMEM((n, out_weight.shape[0], cols), BF16),
            pltpu.VMEM((rows, width), F32),
            pltpu.VMEM((rows, size), F32),
            pltpu.VMEM((rows, size), F32),
            pltpu.VMEM((rows, size), F32),
            pltpu.VMEM((rows, size), F32),
            pltpu.VMEM((rows, size), F32),
            pltpu.VMEM((rows, size), F32),
            pltpu.VMEM((rows, size), F32),
            pltpu.VMEM((HALVES, n, rows // HALVES, size), BF16),
            pltpu.VMEM((HALVES, n, 8, rows), F32),
            dma((6,)),
            dma((n, HALVES)),
            dma((n, HALVES)),
            dma((n,)),
            dma((n,)),
            dma((n, group)),
            dma((n, group)),
            dma((n, HALVES)),
            dma((n, HALVES)),
            dma((n, HALVES)),
            dma((n, HALVES)),
        ],
        compiler_params=pltpu.CompilerParams(collective_id=0, has_side_effects=True),
    )(
        inputs,
        in_weight.reshape(d_model, width),
        gate_weight.reshape(1, d_model),
        gate_bias.reshape(1, 1),
        norm_gain.reshape(1, size),
        out_weight,
        inv_gram.reshape(seqs, size, size),
        value_key.reshape(seqs, size, size),
    )
    return out.reshape(steps, seqs, cols)


def solution(mesh):
    in_specs = (
        P(None, "batch", "head"),
        P(None, "head", None),
        P(None, "head"),
        P("head"),
        P("head"),
        P("head", None),
        P("batch", "head", None, None),
        P("batch", "head", None, None),
    )
    out_specs = P(None, "batch", "head")
    return jax.shard_map(
        functools.partial(local, mesh.shape["head"], mesh.shape["batch"]),
        mesh=mesh,
        in_specs=in_specs,
        out_specs=out_specs,
        check_vma=False,
    )
```

```python
import functools
import math

import jax
import jax.numpy as jnp
from jax import lax
from jax.experimental import pallas as pl
from jax.experimental.pallas import tpu as pltpu
from jax.sharding import PartitionSpec as P

MESH = pl.DeviceIdType.MESH
F32 = jnp.float32
BF16 = jnp.bfloat16
NT = (((1,), (1,)), ((), ()))


def split(x):
    hi = x.astype(BF16)
    lo = (x - hi.astype(F32)).astype(BF16)
    return hi, lo


def rowsum(x):
    return jnp.sum(x, axis=-1, keepdims=True)


def kernel(
    n,
    group,
    x_hbm,
    w_hbm,
    gate_hbm,
    bias_ref,
    gain_ref,
    ow_hbm,
    a_hbm,
    m_hbm,
    out_ref,
    xg,
    w,
    gate,
    a32,
    m32,
    a2,
    m2,
    wout,
    pacc,
    gacc,
    kbuf,
    qbuf,
    akbuf,
    aqbuf,
    wbuf,
    robuf,
    rbuf,
    sqbuf,
    lsem,
    xs,
    xr,
    w1s,
    w1r,
    w2s,
    w2r,
    rs,
    rr,
    qs,
    qr,
):
    steps, seqs, feats = x_hbm.shape
    rows = steps * seqs
    heads_rows = ow_hbm.shape[0]
    cols = ow_hbm.shape[1] // n
    size = a_hbm.shape[1]
    me = lax.axis_index("head")
    b = lax.axis_index("batch")
    mine = lax.rem(b, group)
    base = b - mine
    slab = heads_rows // group

    loads = [
        pltpu.make_async_copy(x_hbm, xg.at[me], lsem.at[0]),
        pltpu.make_async_copy(w_hbm, w, lsem.at[1]),
        pltpu.make_async_copy(gate_hbm, gate, lsem.at[2]),
        pltpu.make_async_copy(a_hbm, a32, lsem.at[3]),
        pltpu.make_async_copy(m_hbm, m32, lsem.at[4]),
        pltpu.make_async_copy(
            ow_hbm.at[:, pl.ds(pl.multiple_of(me * cols, cols), cols)], wout.at[me], lsem.at[5]
        ),
    ]
    for load in loads:
        load.start()

    barrier = pltpu.get_barrier_semaphore()

    for o in range(1, n):
        pl.semaphore_signal(
            barrier, inc=1, device_id={"head": lax.rem(me + o, n)}, device_id_type=MESH
        )
    for o in range(1, group):
        peer = base + lax.rem(mine + o, group)
        pl.semaphore_signal(barrier, inc=1, device_id={"batch": peer}, device_id_type=MESH)
    pl.semaphore_wait(barrier, n + group - 2)

    order = sorted(range(1, n), key=lambda o: -min(o, n - o))

    def xcopy(o):
        return pltpu.make_async_remote_copy(
            src_ref=xg.at[me],
            dst_ref=xg.at[me],
            send_sem=xs.at[o],
            recv_sem=xr.at[o],
            device_id={"head": lax.rem(me + o, n)},
            device_id_type=MESH,
        )

    loads[0].wait()
    for o in order:
        xcopy(o).start()

    def w1copy(o):
        other = lax.rem(me + o, n)
        return pltpu.make_async_remote_copy(
            src_ref=ow_hbm.at[
                pl.ds(pl.multiple_of(mine * slab, slab), slab),
                pl.ds(pl.multiple_of(other * cols, cols), cols),
            ],
            dst_ref=wout.at[me, pl.ds(pl.multiple_of(mine * slab, slab), slab)],
            send_sem=w1s.at[o],
            recv_sem=w1r.at[o],
            device_id={"head": other},
            device_id_type=MESH,
        )

    for o in range(1, n):
        w1copy(o).start()

    def project(j, first):
        x = xg[j].reshape(rows, feats)
        at = pl.ds(pl.multiple_of(j * feats, feats), feats)
        part = jnp.dot(x, w[at, :], preferred_element_type=F32)
        g = jnp.broadcast_to(gate[:, at].astype(F32), (size, feats)).astype(BF16)
        gpart = lax.dot_general(x, g, NT, preferred_element_type=F32)
        if first:
            pacc[...] = part
            gacc[...] = gpart
        else:
            pacc[...] += part
            gacc[...] += gpart

    loads[1].wait()
    loads[2].wait()
    project(me, True)
    loads[3].wait()
    for s in range(seqs):
        hi, lo = split(a32[s])
        a2[s, :size, :] = hi
        a2[s, size:, :] = lo
    loads[4].wait()

    def prepare(start, stop):
        for s in range(start, stop):
            hi, lo = split(m32[s].T)
            m2[s, :size, :] = hi
            m2[s, size:, :] = lo

    for at, o in enumerate(order):
        xcopy(o).wait_recv()
        project(lax.rem(me + n - o, n), False)
        prepare(seqs * at // (n - 1), seqs * (at + 1) // (n - 1))

    p = pacc[...]
    f = 0.8 + 0.2 * jax.nn.sigmoid(gacc[...] + bias_ref[...])
    q = p[:, :size]
    k = p[:, size : 2 * size]
    v = p[:, 2 * size :]
    k = k * lax.rsqrt(rowsum(k * k) + 1e-06)
    q = q * lax.rsqrt(rowsum(q * q) + 1e-06)
    kbuf[...] = k
    qbuf[...] = q
    for s in range(seqs):
        at = pl.ds(s, steps, stride=seqs)
        hi, lo = split(jnp.concatenate([kbuf[at, :], qbuf[at, :]], axis=0))
        left = jnp.concatenate(
            [jnp.concatenate([hi, hi], axis=1), jnp.concatenate([lo, lo], axis=1)], axis=0
        )
        r = jnp.dot(left, a2[s], preferred_element_type=F32)
        r = r[: 2 * steps] + r[2 * steps :]
        akbuf[at, :] = r[:steps]
        aqbuf[at, :] = r[steps:]

    def piece(x, t):
        return x[t * seqs : (t + 1) * seqs]

    ks = [piece(k, t) for t in range(steps)]
    qs_ = [piece(q, t) for t in range(steps)]
    vs = [piece(v, t) for t in range(steps)]
    fs = [piece(f, t) for t in range(steps)]
    ak = [akbuf[t * seqs : (t + 1) * seqs, :] for t in range(steps)]
    aq = [aqbuf[t * seqs : (t + 1) * seqs, :] for t in range(steps)]
    ws = []
    for t in range(steps):
        u = ak[t]
        rd = 1.0 / (fs[t] + rowsum(ks[t] * u))
        rf = 1.0 / fs[t]
        for i in range(t + 1, steps):
            ak[i] = (ak[i] - u * (rowsum(u * ks[i]) * rd)) * rf
        for i in range(t, steps):
            aq[i] = (aq[i] - u * (rowsum(u * qs_[i]) * rd)) * rf
        ws.append(aq[t])
        wbuf[t * seqs : (t + 1) * seqs, :] = aq[t]

    for s in range(seqs):
        at = pl.ds(s, steps, stride=seqs)
        hi, lo = split(wbuf[at, :])
        hi, lo = hi.astype(F32), lo.astype(F32)
        left = jnp.concatenate(
            [jnp.concatenate([hi, hi], axis=1), jnp.concatenate([lo, lo], axis=1)], axis=0
        ).astype(BF16)
        r = jnp.dot(left, m2[s], preferred_element_type=F32)
        robuf[at, :] = r[:steps] + r[steps:]

    decay = []
    whole = None
    pieces = []
    for t in range(steps):
        decay = [x * fs[t] for x in decay] + [None]
        whole = fs[t] if whole is None else whole * fs[t]
        total = whole * robuf[t * seqs : (t + 1) * seqs, :]
        for i in range(t + 1):
            e = rowsum(ks[i] * ws[t])
            total = total + (e * vs[i] if decay[i] is None else (e * decay[i]) * vs[i])
        decay[t] = jnp.ones_like(fs[t])
        pieces.append(total)
    ro = jnp.concatenate(pieces, axis=0)
    hi, lo = split(ro * ro)
    sqbuf[me] = lax.dot_general(
        jnp.ones((8, 2 * size), BF16),
        jnp.concatenate([hi, lo], axis=1),
        NT,
        preferred_element_type=F32,
    )
    rbuf[me] = (gain_ref[...] * ro).astype(BF16)

    def share(buf, send, recv, o):
        return pltpu.make_async_remote_copy(
            src_ref=buf.at[me],
            dst_ref=buf.at[me],
            send_sem=send.at[o],
            recv_sem=recv.at[o],
            device_id={"head": lax.rem(me + o, n)},
            device_id_type=MESH,
        )

    rcopy = functools.partial(share, rbuf, rs, rr)
    qcopy = functools.partial(share, sqbuf, qs, qr)
    for o in range(1, n):
        rcopy(o).start()
        qcopy(o).start()

    def w2copy(o, i):
        source = lax.rem(me + n - o, n)
        part = wout.at[source, pl.ds(pl.multiple_of(mine * slab, slab), slab)]
        return pltpu.make_async_remote_copy(
            src_ref=part,
            dst_ref=part,
            send_sem=w2s.at[o, i],
            recv_sem=w2r.at[o, i],
            device_id={"batch": base + lax.rem(mine + i, group)},
            device_id_type=MESH,
        )

    for o in range(1, n):
        w1copy(o).wait_recv()
        for i in range(1, group):
            w2copy(o, i).start()

    loads[5].wait()
    acc = jnp.dot(rbuf[me], wout[me], preferred_element_type=F32)
    squares = sqbuf[me]
    for o in range(1, n):
        source = lax.rem(me + n - o, n)
        rcopy(o).wait_recv()
        qcopy(o).wait_recv()
        for i in range(1, group):
            w2copy(o, i).wait_recv()
        acc = acc + jnp.dot(rbuf[source], wout[source], preferred_element_type=F32)
        squares = squares + sqbuf[source]
    scale = lax.rsqrt(squares[:1] / (n * size) + 1e-06)
    scale = jnp.broadcast_to(scale, (size, rows)).T
    for at in range(0, cols, size):
        out_ref[:, at : at + size] = acc[:, at : at + size] * scale

    for o in range(1, n):
        xcopy(o).wait_send()
        w1copy(o).wait_send()
        rcopy(o).wait_send()
        qcopy(o).wait_send()
        for i in range(1, group):
            w2copy(o, i).wait_send()


def local(n, batch, inputs, in_weight, gate_weight, gate_bias, norm_gain, out_weight, inv_gram, value_key):
    steps, seqs, feats = inputs.shape
    d_model, heads, width = in_weight.shape
    size = width // 3
    rows = steps * seqs
    cols = out_weight.shape[1] // n
    assert heads == 1
    group = math.gcd(math.gcd(batch, 8), out_weight.shape[0] // 16)
    anywhere = pl.BlockSpec(memory_space=pl.ANY)
    vmem = pl.BlockSpec(memory_space=pltpu.VMEM)
    dma = pltpu.SemaphoreType.DMA
    out = pl.pallas_call(
        functools.partial(kernel, n, group),
        out_shape=jax.ShapeDtypeStruct((rows, cols), F32),
        in_specs=[
            anywhere,
            anywhere,
            anywhere,
            vmem,
            vmem,
            anywhere,
            anywhere,
            anywhere,
        ],
        out_specs=vmem,
        scratch_shapes=[
            pltpu.VMEM((n, steps, seqs, feats), BF16),
            pltpu.VMEM((d_model, width), BF16),
            pltpu.VMEM((1, d_model), BF16),
            pltpu.VMEM((seqs, size, size), F32),
            pltpu.VMEM((seqs, size, size), F32),
            pltpu.VMEM((seqs, 2 * size, size), BF16),
            pltpu.VMEM((seqs, 2 * size, size), BF16),
            pltpu.VMEM((n, out_weight.shape[0], cols), BF16),
            pltpu.VMEM((rows, width), F32),
            pltpu.VMEM((rows, size), F32),
            pltpu.VMEM((rows, size), F32),
            pltpu.VMEM((rows, size), F32),
            pltpu.VMEM((rows, size), F32),
            pltpu.VMEM((rows, size), F32),
            pltpu.VMEM((rows, size), F32),
            pltpu.VMEM((rows, size), F32),
            pltpu.VMEM((n, rows, size), BF16),
            pltpu.VMEM((n, 8, rows), F32),
            dma((6,)),
            dma((n,)),
            dma((n,)),
            dma((n,)),
            dma((n,)),
            dma((n, group)),
            dma((n, group)),
            dma((n,)),
            dma((n,)),
            dma((n,)),
            dma((n,)),
        ],
        compiler_params=pltpu.CompilerParams(collective_id=0, has_side_effects=True),
    )(
        inputs,
        in_weight.reshape(d_model, width),
        gate_weight.reshape(1, d_model),
        gate_bias.reshape(1, 1),
        norm_gain.reshape(1, size),
        out_weight,
        inv_gram.reshape(seqs, size, size),
        value_key.reshape(seqs, size, size),
    )
    return out.reshape(steps, seqs, cols)


def solution(mesh):
    in_specs = (
        P(None, "batch", "head"),
        P(None, "head", None),
        P(None, "head"),
        P("head"),
        P("head"),
        P("head", None),
        P("batch", "head", None, None),
        P("batch", "head", None, None),
    )
    out_specs = P(None, "batch", "head")
    return jax.shard_map(
        functools.partial(local, mesh.shape["head"], mesh.shape["batch"]),
        mesh=mesh,
        in_specs=in_specs,
        out_specs=out_specs,
        check_vma=False,
    )
```
